32 devices in a mesh: dp: 2 (over x), tp: 16 (over z, y, core).
Axes of the slice: x: 2, y: 2, z: 4, core: 2. Of those that a mesh axis runs over, the one named last changes fastest.
Arguments:
- hidden: bfloat16 [4096, 2048], P(('dp', 'tp')), parts along dimension 0
- w_two: bfloat16 [2048, 2048], replicated
- ln_scale: float32 [2, 2048], replicated
- ln_shift: float32 [2, 2048], replicated
- embed: bfloat16 [49152, 2048], P('tp')
- targets: int32 [2, 4096], P(None, ('dp', 'tp')), parts along dimension 1
- loss_mask: int32 [2, 4096], P(None, ('dp', 'tp')), parts along dimension 1
Outputs:
- output 1: float32 [2, 4096], P(None, ('dp', 'tp')), parts along dimension 1
- output 2: float32 [2], P('dp'), parts along dimension 0
- output 3: bfloat16 [4096, 2048], P(('dp', 'tp')), parts along dimension 0
- output 4: float32 [98304, 2048], P(('dp', 'tp')), parts along dimension 0
- output 5: float32 [4096, 2048], P('dp'), parts along dimension 0
- output 6: float32 [4, 2048], P('dp'), parts along dimension 0
- output 7: float32 [4, 2048], P('dp'), parts along dimension 0
There are 2 independent parts. The reference program is written for one: setup_inputs(seed, part) draws one part's arguments, and reference() takes and returns one part's arrays. A program takes and returns all parts, laid end to end along the dimension named above; an argument that names none is the same for every part.
All inputs are finite; a program needn't handle non-finite values.
Results may differ from the reference program's by a relative error of at most 0.0017.
Values are sent between devices in bfloat16 or wider.
A program may use at most 1 GiB of HBM per device.

```python
import math
import jax
import jax.numpy as jnp
from jax import lax

TOKENS_DEV = 128
GROUP_SIZE = 16
D_MODEL = 2048
VOCAB_SIZE = 49152
TABLE_ROWS = 49152

TOKENS = TOKENS_DEV * GROUP_SIZE
ROW_BLOCK = math.gcd(TOKENS, 128)
BLOCKS = TOKENS // ROW_BLOCK
LN_EPS = 1e-5


def setup_inputs(seed: int = 0, part: int = 0) -> dict:
    base = jax.random.key(seed)
    k_w, k_g, k_b, k_e = jax.random.split(base, 4)
    part_key = jax.random.fold_in(base, part)
    k_h, k_t, k_m, k_l = jax.random.split(part_key, 4)
    hidden = jax.random.normal(k_h, (TOKENS, D_MODEL), jnp.float32).astype(jnp.bfloat16)
    w_two = (jax.random.normal(k_w, (D_MODEL, D_MODEL), jnp.float32) * D_MODEL ** -0.5).astype(jnp.bfloat16)
    ln_scale = 1.0 + 0.3 * jax.random.normal(k_g, (2, D_MODEL), jnp.float32)
    ln_shift = 0.3 * jax.random.normal(k_b, (2, D_MODEL), jnp.float32)
    embed = (jax.random.normal(k_e, (TABLE_ROWS, D_MODEL), jnp.float32) * (2.5 * D_MODEL ** -0.5)).astype(jnp.bfloat16)
    targets = jax.random.randint(k_t, (2, TOKENS), 0, VOCAB_SIZE, jnp.int32)
    keep_len = jax.random.randint(k_l, (2, GROUP_SIZE, 1), TOKENS_DEV // 4, TOKENS_DEV + 1, jnp.int32)
    keep_draw = jax.random.randint(k_m, (2, GROUP_SIZE, TOKENS_DEV), 0, 8, jnp.int32)
    position = jnp.arange(TOKENS_DEV, dtype=jnp.int32)
    keep = (position < keep_len) & ((keep_draw != 0) | (position == 0))
    loss_mask = keep.astype(jnp.int32).reshape(2, TOKENS)
    return {'hidden': hidden, 'w_two': w_two, 'ln_scale': ln_scale, 'ln_shift': ln_shift,
            'embed': embed, 'targets': targets, 'loss_mask': loss_mask}


def layer_norm(values, gain, bias):
    mean_val = jnp.mean(values, axis=-1, keepdims=True)
    centered = values - mean_val
    variance = jnp.mean(centered * centered, axis=-1, keepdims=True)
    return centered * lax.rsqrt(variance + LN_EPS) * gain + bias


def reference(hidden, w_two, ln_scale, ln_shift, embed, targets, loss_mask):
    proj_out = jnp.dot(hidden, w_two, preferred_element_type=jnp.float32).astype(jnp.bfloat16)
    norm_input = jnp.stack([hidden.astype(jnp.float32), proj_out.astype(jnp.float32)])
    normed, ln_back = jax.vjp(jax.vmap(layer_norm), norm_input, ln_scale, ln_shift)
    x_both = normed.astype(jnp.bfloat16)
    mask_f = loss_mask.astype(jnp.float32)
    token_count = jnp.sum(mask_f, axis=1)
    weight = mask_f / token_count[:, None]
    x_blocks = jnp.swapaxes(x_both.reshape(2, BLOCKS, ROW_BLOCK, D_MODEL), 0, 1)
    t_blocks = jnp.swapaxes(targets.reshape(2, BLOCKS, ROW_BLOCK), 0, 1)
    w_blocks = jnp.swapaxes(weight.reshape(2, BLOCKS, ROW_BLOCK), 0, 1)
    col_ids = jnp.arange(TABLE_ROWS, dtype=jnp.int32)

    def block_step(d_embed, block):
        x_blk, t_blk, w_blk = block
        raw_rows = []
        dx_rows = []
        for head_idx in range(2):
            logits = jnp.dot(x_blk[head_idx], embed.T, preferred_element_type=jnp.float32)
            log_norm = jax.nn.logsumexp(logits, axis=-1)
            is_target = col_ids[None, :] == t_blk[head_idx][:, None]
            tgt_logit = jnp.sum(jnp.where(is_target, logits, 0.0), axis=-1)
            probs_val = jnp.exp(logits - log_norm[:, None])
            d_logits = ((probs_val - is_target.astype(jnp.float32)) * w_blk[head_idx][:, None]).astype(jnp.bfloat16)
            d_embed = d_embed + jnp.dot(d_logits.T, x_blk[head_idx], preferred_element_type=jnp.float32)
            dx_rows.append(jnp.dot(d_logits, embed, preferred_element_type=jnp.float32))
            raw_rows.append(log_norm - tgt_logit)
        return d_embed, (jnp.stack(raw_rows), jnp.stack(dx_rows))

    d_embed, (raw_loss, d_x) = lax.scan(block_step, jnp.zeros((TABLE_ROWS, D_MODEL), jnp.float32),
                                        (x_blocks, t_blocks, w_blocks))
    raw_loss = jnp.swapaxes(raw_loss, 0, 1).reshape(2, TOKENS)
    d_x = jnp.swapaxes(d_x, 0, 1).reshape(2, TOKENS, D_MODEL)
    token_loss = raw_loss * mask_f
    total_loss = jnp.sum(token_loss / token_count[:, None]).reshape(1)
    d_norm_in, d_ln_scale, d_ln_shift = ln_back(d_x)
    d_proj = d_norm_in[1].astype(jnp.bfloat16)
    d_hidden = (d_norm_in[0] + jnp.dot(d_proj, w_two.T, preferred_element_type=jnp.float32)).astype(jnp.bfloat16)
    d_w_two = jnp.dot(hidden.T, d_proj, preferred_element_type=jnp.float32)
    return token_loss, total_loss, d_hidden, d_embed, d_w_two, d_ln_scale, d_ln_shift
```

```python
import functools
import jax
import jax.numpy as jnp
from jax import lax
from jax.experimental import pallas as pl
from jax.experimental.pallas import tpu as pltpu
from jax.sharding import PartitionSpec as P

LN_EPS = 1e-5
F32 = jnp.float32
BF = jnp.bfloat16
MESH = pl.DeviceIdType.MESH
VMEM_LIMIT = 56 * 1024 * 1024

ALL = [(z, y, c) for z in range(4) for y in range(2) for c in range(2)]


def tp_of(z, y, c):
    return z * 4 + y * 2 + c


CORE_PAIRS = [(tp_of(z, y, c), tp_of(z, y, 1 - c)) for z, y, c in ALL]
Y_PAIRS = [(tp_of(z, y, c), tp_of(z, 1 - y, c)) for z, y, c in ALL]
Z_PAIRS = {k: [(tp_of(z, y, c), tp_of((z + k) % 4, y, c)) for z, y, c in ALL] for k in (1, 2, 3)}


def place():
    me = lax.axis_index('tp')
    return lax.div(me, 4), lax.rem(lax.div(me, 2), 2), lax.rem(me, 2)


def remote(src, dst, send_sem, recv_sem, dev):
    return pltpu.make_async_remote_copy(src_ref=src, dst_ref=dst, send_sem=send_sem, recv_sem=recv_sem,
                                        device_id={'tp': dev}, device_id_type=MESH)


def small_gather_body(x_ref, o_ref, send, recv):
    z, y, c = place()
    barrier = pltpu.get_barrier_semaphore()
    peers = [(r, k) for r in range(4) for k in range(4) if (r, k) != (0, 0)]

    def peer(r, k):
        pz, py, pc = lax.rem(z + k, 4), lax.rem(y + r % 2, 2), lax.rem(c + r // 2, 2)
        return pz, 2 * pc + py, tp_of(pz, py, pc)

    for r, k in peers:
        pl.semaphore_signal(barrier, inc=1, device_id={'tp': peer(r, k)[2]}, device_id_type=MESH)
    pl.semaphore_wait(barrier, len(peers))
    mine = o_ref.at[2 * c + y, z]
    copies = [remote(x_ref, mine, send.at[n], recv.at[r, k], peer(r, k)[2]) for n, (r, k) in enumerate(peers)]
    for copy in copies:
        copy.start()
    o_ref[2 * c + y, z] = x_ref[...]
    for n, (r, k) in enumerate(peers):
        pz, pq, dev = peer(r, 4 - k)
        remote(x_ref, o_ref.at[pq, pz], send.at[n], recv.at[r, k], dev).wait_recv()
    for copy in copies:
        copy.wait_send()


def small_gather(x, cid):
    return pl.pallas_call(
        small_gather_body, out_shape=jax.ShapeDtypeStruct((4, 4) + x.shape, x.dtype),
        in_specs=[pl.BlockSpec(memory_space=pltpu.VMEM)], out_specs=pl.BlockSpec(memory_space=pltpu.VMEM),
        scratch_shapes=[pltpu.SemaphoreType.DMA((15,)), pltpu.SemaphoreType.DMA((4, 4))],
        compiler_params=pltpu.CompilerParams(collective_id=cid, has_side_effects=True))(x)


def row_gather_body(x_ref, o_ref, up_s, dn_s, y_s, c_s, recv):
    z, y, c = place()
    barrier = pltpu.get_barrier_semaphore()
    me = tp_of(z, y, c)
    y_dev, c_dev = tp_of(z, 1 - y, c), tp_of(z, y, 1 - c)
    has_up, has_dn = z < 3, z > 0

    def greet(dev):
        pl.semaphore_signal(barrier, inc=1, device_id={'tp': dev}, device_id_type=MESH)

    greet(y_dev)
    greet(c_dev)
    pl.when(has_up)(lambda: greet(me + 4))
    pl.when(has_dn)(lambda: greet(me - 4))
    pl.semaphore_wait(barrier, 2 + has_up.astype(jnp.int32) + has_dn.astype(jnp.int32))

    q, qy = 2 * c + y, 2 * c + 1 - y
    quarter = [q, qy, 2 * (1 - c) + y, 2 * (1 - c) + 1 - y]

    def up(src, b):
        return remote(src, o_ref.at[q, b], up_s.at[b], recv.at[0, b], me + 4)

    def dn(src, b):
        return remote(src, o_ref.at[q, b], dn_s.at[b], recv.at[0, b], me - 4)

    def ycopy(src, b):
        return remote(src, o_ref.at[q, b], y_s.at[b], recv.at[1, b], y_dev)

    def ccopy(src, r, b):
        return remote(src, o_ref.at[quarter[r], b], c_s.at[r, b], recv.at[r + 2, b], c_dev)

    def landed(r, b):
        remote(x_ref, o_ref.at[quarter[r], b], c_s.at[0, b], recv.at[r, b], c_dev).wait_recv()

    pl.when(has_up)(lambda: up(x_ref, z).start())
    pl.when(has_dn)(lambda: dn(x_ref, z).start())
    ycopy(x_ref, z).start()
    ccopy(x_ref, 0, z).start()
    o_ref[q, z] = x_ref[...]
    for k in (1, 2, 3):
        lo, hi = z - k, z + k

        @pl.when(lo >= 0)
        def _():
            landed(0, lo)
            pl.when(has_up)(lambda: up(o_ref.at[q, lo], lo).start())
            ycopy(o_ref.at[q, lo], lo).start()
            ccopy(o_ref.at[q, lo], 0, lo).start()

        @pl.when(hi <= 3)
        def _():
            landed(0, hi)
            pl.when(has_dn)(lambda: dn(o_ref.at[q, hi], hi).start())
            ycopy(o_ref.at[q, hi], hi).start()
            ccopy(o_ref.at[q, hi], 0, hi).start()
    for k in range(4):
        for b, ok in ((z - k, z - k >= 0), (z + k, z + k <= 3)) if k else ((z, z >= 0),):
            @pl.when(ok)
            def _():
                landed(1, b)
                ccopy(o_ref.at[qy, b], 1, b).start()
    for b in range(4):
        landed(2, b)
        landed(3, b)
    for b in range(4):
        pl.when(has_up & (z >= b))(lambda: up(o_ref.at[q, b], b).wait_send())
        pl.when(has_dn & (z <= b))(lambda: dn(o_ref.at[q, b], b).wait_send())
        ycopy(o_ref.at[q, b], b).wait_send()
        ccopy(o_ref.at[q, b], 0, b).wait_send()
        ccopy(o_ref.at[qy, b], 1, b).wait_send()


def row_gather(x, cid):
    return pl.pallas_call(
        row_gather_body, out_shape=jax.ShapeDtypeStruct((4, 4) + x.shape, x.dtype),
        in_specs=[pl.BlockSpec(memory_space=pltpu.VMEM)], out_specs=pl.BlockSpec(memory_space=pltpu.VMEM),
        scratch_shapes=[pltpu.SemaphoreType.DMA((4,)), pltpu.SemaphoreType.DMA((4,)), pltpu.SemaphoreType.DMA((4,)),
                        pltpu.SemaphoreType.DMA((2, 4)), pltpu.SemaphoreType.DMA((4, 4))],
        compiler_params=pltpu.CompilerParams(collective_id=cid, has_side_effects=True, vmem_limit_bytes=16 * 1024 * 1024),
        cost_estimate=pl.CostEstimate(flops=30_000_000_000, bytes_accessed=2 * 16 * x.size, transcendentals=0))(x)


def logits_body(chunk, x_ref, e_ref, t_ref, z_ref, s_ref):
    tm = x_ref.shape[0]
    vocab = e_ref.shape[0]
    x = x_ref[...]
    tgt = t_ref[...].T[:, 0:1].astype(jnp.int32)
    m = s = t = None
    lane = lax.broadcasted_iota(jnp.int32, (tm, 128), 1)
    for j in range(vocab // chunk):
        z = lax.dot_general(x, e_ref[pl.ds(j * chunk, chunk), :], (((1,), (1,)), ((), ())), preferred_element_type=F32)
        z_ref[:, pl.ds(j * chunk, chunk)] = z
        parts = [z[:, k * 128:(k + 1) * 128] for k in range(chunk // 128)]
        hits = [jnp.where(lane == tgt - (j * chunk + k * 128), p, 0.0) for k, p in enumerate(parts)]
        n = functools.reduce(jnp.maximum, parts if m is None else [m] + parts)
        add = functools.reduce(jnp.add, [jnp.exp(p - n) for p in parts])
        s = add if m is None else s * jnp.exp(m - n) + add
        t = functools.reduce(jnp.add, hits if t is None else [t] + hits)
        m = n
    mx = jnp.max(m, axis=1, keepdims=True)
    sm = jnp.sum(s * jnp.exp(m - mx), axis=1, keepdims=True)
    tt = jnp.sum(t, axis=1, keepdims=True)
    s_ref[...] = jnp.where(lane == 0, mx, jnp.where(lane == 1, sm, tt)).T[:8, :]


def logits_call(x, e, rows8):
    b, d = x.shape
    v = e.shape[0]
    tm = 256
    return pl.pallas_call(
        functools.partial(logits_body, 512), grid=(b // tm,),
        in_specs=[pl.BlockSpec((tm, d), lambda i: (i, 0)),
                  pl.BlockSpec((v, d), lambda i: (0, 0), pipeline_mode=pl.Buffered(1)),
                  pl.BlockSpec((8, tm), lambda i: (0, i))],
        out_specs=[pl.BlockSpec((tm, v), lambda i: (i, 0)), pl.BlockSpec((8, tm), lambda i: (0, i))],
        out_shape=[jax.ShapeDtypeStruct((b, v), F32), jax.ShapeDtypeStruct((8, b), F32)],
        compiler_params=pltpu.CompilerParams(vmem_limit_bytes=VMEM_LIMIT),
        cost_estimate=pl.CostEstimate(flops=2 * b * d * v, bytes_accessed=4 * b * v, transcendentals=b * v))(x, e, rows8)


def grad_body(sub, nb, perm, z_ref, e_ref, r_ref, dz_ref, c_ref, y_ref, o_ref):
    tm, v = z_ref.shape
    i = pl.program_id(0)
    cols = r_ref[...].T
    res = []
    for a in range(tm // sub):
        r = pl.ds(a * sub, sub)
        lse, w, tgt = [cols[a * sub:(a + 1) * sub, k:k + 1] for k in range(3)]
        p = jnp.exp(z_ref[r, :] - lse)
        lane = lax.broadcasted_iota(jnp.int32, (sub, v), 1)
        p = jnp.where(lane == tgt.astype(jnp.int32), p - 1.0, p)
        dz = (p * w).astype(BF)
        dz_ref[r, :] = dz
        res.append(jnp.dot(dz, e_ref[...], preferred_element_type=F32))

    def put(ref):
        for a, val in enumerate(res):
            ref[pl.ds(a * sub, sub), :] = val

    pl.when(i < 2 * nb)(lambda: put(c_ref))
    pl.when((i >= 2 * nb) & (i < 3 * nb))(lambda: put(y_ref))
    pl.when(i >= 3 * nb)(lambda: put(o_ref))


def grad_call(z, e, rows8, perm):
    b, v = z.shape
    d = e.shape[1]
    tm = TM_GRAD
    nb = b // 4 // tm
    row = lambda i, p: (p[lax.div(i, nb)] * nb + lax.rem(i, nb), 0)
    return pl.pallas_call(
        functools.partial(grad_body, 128, nb),
        grid_spec=pltpu.PrefetchScalarGridSpec(
            num_scalar_prefetch=1, grid=(b // tm,),
            in_specs=[pl.BlockSpec((tm, v), row),
                      pl.BlockSpec((v, d), lambda i, p: (0, 0), pipeline_mode=pl.Buffered(1)),
                      pl.BlockSpec((8, tm), lambda i, p: row(i, p)[::-1])],
            out_specs=[pl.BlockSpec((tm, v), row),
                       pl.BlockSpec((tm, d), lambda i, p: (jnp.minimum(i, 2 * nb - 1), 0)),
                       pl.BlockSpec((tm, d), lambda i, p: (jnp.clip(i - 2 * nb, 0, nb - 1), 0)),
                       pl.BlockSpec((tm, d), lambda i, p: (jnp.clip(i - 3 * nb, 0, nb - 1), 0))]),
        out_shape=[jax.ShapeDtypeStruct((b, v), BF), jax.ShapeDtypeStruct((b // 2, d), F32),
                   jax.ShapeDtypeStruct((b // 4, d), F32), jax.ShapeDtypeStruct((b // 4, d), F32)],
        compiler_params=pltpu.CompilerParams(vmem_limit_bytes=VMEM_LIMIT),
        cost_estimate=pl.CostEstimate(flops=2 * b * d * v, bytes_accessed=6 * b * v,
                                      transcendentals=b * v))(perm, z, e, rows8)


TN = (((0,), (0,)), ((), ()))


def embed_body(a_ref, b_ref, xa_ref, xb_ref, o_ref):
    o_ref[...] = lax.dot_general(a_ref[...], xa_ref[...], TN, preferred_element_type=F32)
    o_ref[...] += lax.dot_general(b_ref[...], xb_ref[...], TN, preferred_element_type=F32)


def embed_call(da, db, xa, xb):
    b, v = da.shape
    d = xa.shape[1]
    tv = 256
    col = pl.BlockSpec((b, tv), lambda j: (0, j))
    full = pl.BlockSpec((b, d), lambda j: (0, 0), pipeline_mode=pl.Buffered(1))
    return pl.pallas_call(
        embed_body, grid=(v // tv,), in_specs=[col, col, full, full],
        out_specs=pl.BlockSpec((tv, d), lambda j: (j, 0)), out_shape=jax.ShapeDtypeStruct((v, d), F32),
        compiler_params=pltpu.CompilerParams(vmem_limit_bytes=VMEM_LIMIT),
        cost_estimate=pl.CostEstimate(flops=4 * b * d * v, bytes_accessed=4 * b * v, transcendentals=0))(da, db, xa, xb)


def weight_body(h_ref, g_ref, o_ref):
    o_ref[...] = lax.dot_general(h_ref[...], g_ref[...], TN, preferred_element_type=F32)


def weight_call(h, g):
    t, d = h.shape
    tv = 256
    return pl.pallas_call(
        weight_body, grid=(d // tv,),
        in_specs=[pl.BlockSpec((t, tv), lambda j: (0, j)),
                  pl.BlockSpec((t, d), lambda j: (0, 0), pipeline_mode=pl.Buffered(1))],
        out_specs=pl.BlockSpec((tv, d), lambda j: (j, 0)), out_shape=jax.ShapeDtypeStruct((d, d), F32),
        compiler_params=pltpu.CompilerParams(vmem_limit_bytes=VMEM_LIMIT),
        cost_estimate=pl.CostEstimate(flops=2 * t * d * d, bytes_accessed=4 * d * d, transcendentals=0))(h, g)


def layer_norm(values, gain, bias):
    mean_val = jnp.mean(values, axis=-1, keepdims=True)
    centered = values - mean_val
    variance = jnp.mean(centered * centered, axis=-1, keepdims=True)
    return centered * lax.rsqrt(variance + LN_EPS) * gain + bias


def norm_back_body(p0, p1, p2, p3, a_ref, g_ref, da_ref, db_ref, s_ref):
    dy = (p0[...] + p1[...]) + (p2[...] + p3[...])
    a = a_ref[...].astype(F32)
    cen = a - jnp.mean(a, axis=1, keepdims=True)
    inv = lax.rsqrt(jnp.mean(cen * cen, axis=1, keepdims=True) + LN_EPS)
    hat = cen * inv
    dh = dy * g_ref[...]
    da = inv * (dh - jnp.mean(dh, axis=1, keepdims=True) - hat * jnp.mean(dh * hat, axis=1, keepdims=True))
    da_ref[...] = da
    db_ref[...] = da.astype(BF)
    ds = jnp.sum(dy * hat, axis=0, keepdims=True)
    dt = jnp.sum(dy, axis=0, keepdims=True)
    row = lax.broadcasted_iota(jnp.int32, s_ref.shape, 0)
    s_ref[...] = jnp.where(row == 0, ds, jnp.where(row == 1, dt, 0.0))


def norm_back(parts, a, gain):
    t, d = a.shape
    vm = pl.BlockSpec(memory_space=pltpu.VMEM)
    return pl.pallas_call(
        norm_back_body, in_specs=[vm] * 6, out_specs=[vm] * 3,
        out_shape=[jax.ShapeDtypeStruct((t, d), F32), jax.ShapeDtypeStruct((t, d), BF), jax.ShapeDtypeStruct((8, d), F32)],
        compiler_params=pltpu.CompilerParams(vmem_limit_bytes=24 * 1024 * 1024),
        cost_estimate=pl.CostEstimate(flops=1_000_000_000, bytes_accessed=22 * t * d, transcendentals=t))(*parts, a, gain)


TM_GRAD = 256


def solution(mesh):
    tok_spec = P(('dp', 'tp'), None)
    row_spec = P(None, ('dp', 'tp'))

    def step(hidden, w_two, ln_scale, ln_shift, embed, targets, loss_mask):
        toks, width = hidden.shape
        shard_rows = embed.shape[0]
        zi, yi, ci = place()
        base = (lax.axis_index('tp') * shard_rows).astype(F32)
        mine = 2 * ci + yi
        perm = jnp.stack([3 - mine, 2 * (1 - ci) + yi, 2 * ci + 1 - yi, mine])
        ints = small_gather(jnp.concatenate([targets, loss_mask, jnp.zeros((4, toks), jnp.int32)], axis=0), 1)
        h_all = row_gather(hidden, 2).reshape(16 * toks, width)
        mask = [ints[:, :, 2 + h].astype(F32).reshape(-1) for h in range(2)]
        count = [jnp.sum(m) for m in mask]

        def forward(h, a, cid):
            x = layer_norm(a.astype(F32), ln_scale[h], ln_shift[h]).astype(BF)
            tgt = ints[:, :, h].reshape(-1).astype(F32) - base
            z, st = logits_call(x, embed, jnp.broadcast_to(tgt, (8, tgt.shape[0])))
            part = jnp.concatenate([(st[0] + jnp.log(st[1])).reshape(-1, 128), st[2].reshape(-1, 128)], axis=0)
            parts = small_gather(part, cid).reshape(16, 2, -1, 128)
            top = jnp.max(parts[:, 0], axis=0)
            lse = top + jnp.log(jnp.sum(jnp.exp(parts[:, 0] - top), axis=0))
            raw = (lse - jnp.sum(parts[:, 1], axis=0)).reshape(-1)
            wgt = mask[h] / count[h]
            rows8 = jnp.concatenate([jnp.stack([lse.reshape(-1), wgt, tgt]), jnp.zeros((5, tgt.shape[0]), F32)], axis=0)
            dz, to_core, to_y, own = grad_call(z, embed, rows8, perm)
            loss = raw * mask[h]
            own_loss = lax.dynamic_slice_in_dim(loss, (mine * 4 + zi) * toks, toks)
            return x, dz, (to_core, to_y, own), own_loss, jnp.sum(loss / count[h])

        def exchange(to_core, to_y, own):
            n = own.shape[0]
            from_core = lax.ppermute(to_core, 'tp', CORE_PAIRS)
            halves = []
            for k in range(2):
                rows = slice(k * n // 2, (k + 1) * n // 2)
                send = to_y[rows] + from_core[:n][rows]
                halves.append(own[rows] + from_core[n:][rows] + lax.ppermute(send, 'tp', Y_PAIRS))
            part = jnp.concatenate(halves, axis=0).reshape(4, toks, width)
            parts = [lax.dynamic_index_in_dim(part, zi, 0, keepdims=False)]
            for k in (1, 2, 3):
                block = lax.dynamic_index_in_dim(part, lax.rem(zi + k, 4), 0, keepdims=False)
                parts.append(lax.ppermute(block, 'tp', Z_PAIRS[k]))
            return parts

        a_all = jnp.dot(h_all, w_two, preferred_element_type=F32).astype(BF)
        x_b, dz_b, send_b, loss_b, tot_b = forward(1, a_all, 3)
        dx_b = exchange(*send_b)
        h_one, _ = lax.optimization_barrier((h_all, send_b[2]))
        x_a, dz_a, send_a, loss_a, tot_a = forward(0, h_one, 4)
        dx_a = exchange(*send_a)
        d_embed = embed_call(dz_a, dz_b, x_a, x_b)

        proj_loc = jnp.dot(hidden, w_two, preferred_element_type=F32).astype(BF)
        _, d_proj, sums_b = norm_back(dx_b, proj_loc, ln_scale[1:2])
        g_all = row_gather(d_proj, 5).reshape(16 * toks, width)
        d_w_two = weight_call(h_all, g_all)
        via_two = lax.dot_general(d_proj, w_two, (((1,), (1,)), ((), ())), preferred_element_type=F32)
        da_a, _, sums_a = norm_back(dx_a, hidden, ln_scale[0:1])
        d_hidden = (da_a + via_two).astype(BF)
        ln_part = jnp.concatenate([v.reshape(-1, 128) for v in (sums_a[0], sums_b[0], sums_a[1], sums_b[1])], axis=0)
        ln_all = jnp.sum(small_gather(ln_part, 6).reshape(16, 4, width), axis=0)
        token_loss = jnp.stack([loss_a, loss_b])
        return token_loss, (tot_a + tot_b).reshape(1), d_hidden, d_embed, d_w_two, ln_all[:2], ln_all[2:]

    return jax.shard_map(step, mesh=mesh,
                         in_specs=(tok_spec, P(), P(), P(), P('tp', None), row_spec, row_spec),
                         out_specs=(row_spec, P('dp'), tok_spec, tok_spec, P('dp', None), P('dp', None), P('dp', None)),
                         check_vma=False)
```

```python
import functools
import jax
import jax.numpy as jnp
from jax import lax
from jax.experimental import pallas as pl
from jax.experimental.pallas import tpu as pltpu
from jax.sharding import PartitionSpec as P

LN_EPS = 1e-5
F32 = jnp.float32
BF = jnp.bfloat16
MESH = pl.DeviceIdType.MESH
VMEM_LIMIT = 56 * 1024 * 1024

ALL = [(z, y, c) for z in range(4) for y in range(2) for c in range(2)]


def tp_of(z, y, c):
    return z * 4 + y * 2 + c


CORE_PAIRS = [(tp_of(z, y, c), tp_of(z, y, 1 - c)) for z, y, c in ALL]
Y_PAIRS = [(tp_of(z, y, c), tp_of(z, 1 - y, c)) for z, y, c in ALL]
Z_PAIRS = {k: [(tp_of(z, y, c), tp_of((z + k) % 4, y, c)) for z, y, c in ALL] for k in (1, 2, 3)}


def place():
    me = lax.axis_index('tp')
    return lax.div(me, 4), lax.rem(lax.div(me, 2), 2), lax.rem(me, 2)


def remote(src, dst, send_sem, recv_sem, dev):
    return pltpu.make_async_remote_copy(src_ref=src, dst_ref=dst, send_sem=send_sem, recv_sem=recv_sem,
                                        device_id={'tp': dev}, device_id_type=MESH)


def direct_exchange(both, x_ref, o_ref, send, recv):
    z, y, c = place()
    d = lax.axis_index('dp')
    peers = [(g, r, k) for g in range(1 + both) for r in range(4) for k in range(4)][1:]
    slot = (d if both else 0, 2 * c + y, z)

    def peer(g, r, k):
        pg, pz, py, pc = lax.rem(d + g, 2), lax.rem(z + k, 4), lax.rem(y + r % 2, 2), lax.rem(c + r // 2, 2)
        return {'dp': pg, 'tp': tp_of(pz, py, pc)}, (pg if both else 0, 2 * pc + py, pz)

    def copy(n, p, at, dev):
        return pltpu.make_async_remote_copy(src_ref=x_ref, dst_ref=o_ref.at[at], send_sem=send.at[n], recv_sem=recv.at[p],
                                            device_id=dev, device_id_type=MESH)

    def greets():
        barrier = pltpu.get_barrier_semaphore()
        for p in peers:
            pl.semaphore_signal(barrier, inc=1, device_id=peer(*p)[0], device_id_type=MESH)
        pl.semaphore_wait(barrier, len(peers))

    def start():
        for n, p in enumerate(peers):
            copy(n, p, slot, peer(*p)[0]).start()
        o_ref[slot] = x_ref[...]

    def end():
        for n, p in enumerate(peers):
            dev, at = peer(p[0], p[1], 4 - p[2])
            copy(n, p, at, dev).wait_recv()
        for n, p in enumerate(peers):
            copy(n, p, slot, peer(*p)[0]).wait_send()

    return greets, start, end


def small_gather_body(x_ref, o_ref, send, recv):
    for part in direct_exchange(0, x_ref, o_ref, send, recv):
        part()


def small_gather(x, cid):
    return pl.pallas_call(
        small_gather_body, out_shape=jax.ShapeDtypeStruct((1, 4, 4) + x.shape, x.dtype),
        in_specs=[pl.BlockSpec(memory_space=pltpu.VMEM)], out_specs=pl.BlockSpec(memory_space=pltpu.VMEM),
        scratch_shapes=[pltpu.SemaphoreType.DMA((15,)), pltpu.SemaphoreType.DMA((1, 4, 4))],
        compiler_params=pltpu.CompilerParams(collective_id=cid, has_side_effects=True))(x)[0]


def row_gather_body(both, x_ref, i_ref, o_ref, a_ref, up_s, dn_s, y_s, c_s, recv, isend, irecv):
    greets, ints_start, ints_end = direct_exchange(both, i_ref, a_ref, isend, irecv)
    z, y, c = place()
    me = tp_of(z, y, c)
    y_dev, c_dev = tp_of(z, 1 - y, c), tp_of(z, y, 1 - c)
    has_up, has_dn = z < 3, z > 0

    greets()
    q, qy = 2 * c + y, 2 * c + 1 - y
    quarter = [q, qy, 2 * (1 - c) + y, 2 * (1 - c) + 1 - y]

    def up(src, b):
        return remote(src, o_ref.at[q, b], up_s.at[b], recv.at[0, b], me + 4)

    def dn(src, b):
        return remote(src, o_ref.at[q, b], dn_s.at[b], recv.at[0, b], me - 4)

    def ycopy(src, b):
        return remote(src, o_ref.at[q, b], y_s.at[b], recv.at[1, b], y_dev)

    def ccopy(src, r, b):
        return remote(src, o_ref.at[quarter[r], b], c_s.at[r, b], recv.at[r + 2, b], c_dev)

    def landed(r, b):
        remote(x_ref, o_ref.at[quarter[r], b], c_s.at[0, b], recv.at[r, b], c_dev).wait_recv()

    pl.when(has_up)(lambda: up(x_ref, z).start())
    pl.when(has_dn)(lambda: dn(x_ref, z).start())
    ycopy(x_ref, z).start()
    ccopy(x_ref, 0, z).start()
    ints_start()
    o_ref[q, z] = x_ref[...]
    for k in (1, 2, 3):
        lo, hi = z - k, z + k

        @pl.when(lo >= 0)
        def _():
            landed(0, lo)
            pl.when(has_up)(lambda: up(o_ref.at[q, lo], lo).start())
            ycopy(o_ref.at[q, lo], lo).start()
            ccopy(o_ref.at[q, lo], 0, lo).start()

        @pl.when(hi <= 3)
        def _():
            landed(0, hi)
            pl.when(has_dn)(lambda: dn(o_ref.at[q, hi], hi).start())
            ycopy(o_ref.at[q, hi], hi).start()
            ccopy(o_ref.at[q, hi], 0, hi).start()
    for k in range(4):
        for b, ok in ((z - k, z - k >= 0), (z + k, z + k <= 3)) if k else ((z, z >= 0),):
            @pl.when(ok)
            def _():
                landed(1, b)
                ccopy(o_ref.at[qy, b], 1, b).start()
    for b in range(4):
        landed(2, b)
        landed(3, b)
    for b in range(4):
        pl.when(has_up & (z >= b))(lambda: up(o_ref.at[q, b], b).wait_send())
        pl.when(has_dn & (z <= b))(lambda: dn(o_ref.at[q, b], b).wait_send())
        ycopy(o_ref.at[q, b], b).wait_send()
        ccopy(o_ref.at[q, b], 0, b).wait_send()
        ccopy(o_ref.at[qy, b], 1, b).wait_send()
    ints_end()


def row_gather(x, cid, ints, both):
    vm = pl.BlockSpec(memory_space=pltpu.VMEM)
    dma = pltpu.SemaphoreType.DMA
    more = [ints]
    outs = [jax.ShapeDtypeStruct((4, 4) + x.shape, x.dtype)] + [jax.ShapeDtypeStruct((1 + both, 4, 4) + i.shape, i.dtype) for i in more]
    out = pl.pallas_call(
        functools.partial(row_gather_body, both), out_shape=outs,
        in_specs=[vm] * len(outs), out_specs=[vm] * len(outs),
        scratch_shapes=[dma((4,))] * 3 + [dma((2, 4)), dma((4, 4))] + [dma((16 * both + 15,)), dma((1 + both, 4, 4))],
        compiler_params=pltpu.CompilerParams(collective_id=cid, has_side_effects=True, vmem_limit_bytes=16 * 1024 * 1024),
        cost_estimate=cost(30_000_000_000, 32 * x.size))(x, *more)
    return out


NT = (((1,), (1,)), ((), ()))
TN = (((0,), (0,)), ((), ()))


def fixed(shape, **kw):
    at = tuple(0 for _ in shape)
    return pl.BlockSpec(shape, lambda *_: at, **kw)


def once(shape):
    return fixed(shape, pipeline_mode=pl.Buffered(1))


def cost(flops, data):
    return pl.CostEstimate(flops=flops, bytes_accessed=data, transcendentals=0)


def row_mean(v):
    return jnp.mean(v, axis=1, keepdims=True)


def columns(values, width=128):
    lane = lax.broadcasted_iota(jnp.int32, (values[0].shape[0], width), 1)
    out = jnp.zeros(lane.shape, F32)
    for n, v in enumerate(values):
        out = jnp.where(lane == n, v, out)
    return out


def logits_body(chunk, h_ref, e_ref, t_ref, g_ref, z_ref, s_ref, x_ref, scr):
    tm = h_ref.shape[0]
    vocab = e_ref.shape[0]
    tgt = t_ref[0].T[:tm, 0:1].astype(jnp.int32)
    lane = lax.broadcasted_iota(jnp.int32, (tm, 128), 1)
    cen = h_ref[...].astype(F32)
    mean = row_mean(cen)
    cen = cen - mean
    inv = lax.rsqrt(row_mean(cen * cen) + LN_EPS)
    x = (cen * inv * g_ref[0:1, :] + g_ref[1:2, :]).astype(BF)
    x_ref[...] = x
    m = s = t = None
    for j in range(vocab // chunk):
        z = lax.dot_general(x, e_ref[pl.ds(j * chunk, chunk), :], NT, preferred_element_type=F32)
        z_ref[:, pl.ds(j * chunk, chunk)] = z
        parts = [z[:, k * 128:(k + 1) * 128] for k in range(chunk // 128)]
        hits = [jnp.where(lane == tgt - (j * chunk + k * 128), p, 0.0) for k, p in enumerate(parts)]
        n = functools.reduce(jnp.maximum, parts if m is None else [m] + parts)
        add = functools.reduce(jnp.add, [jnp.exp(p - n) for p in parts])
        s = add if m is None else s * jnp.exp(m - n) + add
        t = functools.reduce(jnp.add, hits if t is None else [t] + hits)
        m = n
    mx = jnp.max(m, axis=1, keepdims=True)
    sm = jnp.sum(s * jnp.exp(m - mx), axis=1, keepdims=True)
    tt = jnp.sum(t, axis=1, keepdims=True)
    scr[...] = jnp.zeros_like(scr)
    scr[:tm, :] = columns((mx, sm, tt, mean, inv))
    s_ref[0] = scr[...].T[:8, :]


def logits_call(h, e, rows8, gain):
    b, d = h.shape
    v = e.shape[0]
    tm = b // 4
    row = pl.BlockSpec((tm, d), lambda i: (i, 0))
    stat = pl.BlockSpec((1, 8, 512), lambda i: (i, 0, 0))
    return pl.pallas_call(
        functools.partial(logits_body, 512), grid=(4,),
        in_specs=[row, once((v, d)), stat, fixed(gain.shape)],
        out_specs=[pl.BlockSpec((tm, v), lambda i: (i, 0)), stat, row],
        out_shape=[jax.ShapeDtypeStruct((b, v), F32), jax.ShapeDtypeStruct((4, 8, 512), F32), jax.ShapeDtypeStruct((b, d), BF)],
        scratch_shapes=[pltpu.VMEM((512, 128), F32)],
        compiler_params=pltpu.CompilerParams(vmem_limit_bytes=VMEM_LIMIT),
        cost_estimate=cost(2 * b * d * v, 4 * b * v))(h, e, rows8, gain)


def put_rows(val, c_ref, y_ref, o_ref):
    i = pl.program_id(0)
    for ok, ref in ((i < 2, c_ref), (i == 2, y_ref), (i == 3, o_ref)):
        @pl.when(ok)
        def _():
            ref[...] = val[...]


def norm_sums(acc, h_ref, cols, s_ref):
    tm = acc.shape[0]
    hat = (h_ref[...].astype(F32) - cols[:tm, 3:4]) * cols[:tm, 4:5]
    ds = jnp.sum(acc[...] * hat, axis=0, keepdims=True)
    dt = jnp.sum(acc[...], axis=0, keepdims=True)
    row = lax.broadcasted_iota(jnp.int32, s_ref.shape, 0)
    new = jnp.where(row == 0, ds, jnp.where(row == 1, dt, 0.0))

    @pl.when(pl.program_id(0) == 0)
    def _():
        s_ref[...] = new

    @pl.when(pl.program_id(0) > 0)
    def _():
        s_ref[...] += new


def grad_body(perm, z_ref, e_ref, r_ref, h_ref, dz_ref, c_ref, y_ref, o_ref, s_ref, acc):
    tm, v = z_ref.shape
    cols = r_ref[0].T
    lse, w, tgt = [cols[:tm, k:k + 1] for k in range(3)]
    tgt = tgt.astype(jnp.int32)
    lane = lax.broadcasted_iota(jnp.int32, (tm, 512), 1)
    for j in range(v // 512):
        p = jnp.exp(z_ref[:, j * 512:(j + 1) * 512] - lse)
        p = jnp.where(lane == tgt - j * 512, p - 1.0, p)
        dz_ref[:, j * 512:(j + 1) * 512] = (p * w).astype(BF)
    acc[...] = jnp.dot(dz_ref[...], e_ref[...], preferred_element_type=F32)
    put_rows(acc, c_ref, y_ref, o_ref)
    norm_sums(acc, h_ref, cols, s_ref)


def half_body(perm, z_ref, e_ref, r_ref, h_ref, c_ref, y_ref, o_ref, s_ref, acc):
    acc[...] = jnp.dot(z_ref[...], e_ref[...], preferred_element_type=F32)
    put_rows(acc, c_ref, y_ref, o_ref)
    norm_sums(acc, h_ref, r_ref[0].T, s_ref)


def grad_call(first, z, e, rows8, hid, perm):
    b, v = z.shape
    d = e.shape[1] // 2
    tm = b // 4
    half = 0 if first else 1
    row = pl.BlockSpec((tm, v), lambda i, p: (p[i], 0))
    outs = [pl.BlockSpec((tm, d), lambda i, p: (jnp.minimum(i, 1), 0)), fixed((tm, d)), fixed((tm, d)),
            fixed((8, d))]
    shapes = [jax.ShapeDtypeStruct((b // 2, d), F32), jax.ShapeDtypeStruct((b // 4, d), F32),
              jax.ShapeDtypeStruct((b // 4, d), F32), jax.ShapeDtypeStruct((8, d), F32)]
    return pl.pallas_call(
        grad_body if first else half_body,
        grid_spec=pltpu.PrefetchScalarGridSpec(
            num_scalar_prefetch=1, grid=(4,),
            in_specs=[row, pl.BlockSpec((v, d), lambda i, p: (0, half), pipeline_mode=pl.Buffered(1)),
                      pl.BlockSpec((1, 8, 512), lambda i, p: (p[i], 0, 0)),
                      pl.BlockSpec((tm, d), lambda i, p: (p[i], half))],
            out_specs=[row] * first + outs, scratch_shapes=[pltpu.VMEM((tm, d), F32)]),
        out_shape=[jax.ShapeDtypeStruct((b, v), BF)] * first + shapes,
        compiler_params=pltpu.CompilerParams(vmem_limit_bytes=VMEM_LIMIT),
        cost_estimate=cost(2 * b * d * v, 2 * b * v))(perm, z, e, rows8, hid)


def embed_body(a_ref, b_ref, xa_ref, xb_ref, o_ref):
    o_ref[...] = lax.dot_general(a_ref[...], xa_ref[...], TN, preferred_element_type=F32)
    o_ref[...] += lax.dot_general(b_ref[...], xb_ref[...], TN, preferred_element_type=F32)


def embed_call(da, db, xa, xb, half, into=None):
    v = da.shape[1]
    d = xa.shape[1]
    tv = 256
    n = v // tv // 2

    def body(*refs):
        embed_body(*refs[:4], refs[-1])

    def col(x):
        return pl.BlockSpec((x.shape[0], tv), lambda j: (0, half * n + j))

    def full(x):
        return once(x.shape)

    more = [] if into is None else [into]
    return pl.pallas_call(
        body, grid=(n,), in_specs=[col(da), col(db), full(xa), full(xb)] + [pl.BlockSpec(memory_space=pl.ANY) for _ in more],
        out_specs=pl.BlockSpec((tv, d), lambda j: (half * n + j, 0)), out_shape=jax.ShapeDtypeStruct((v, d), F32),
        input_output_aliases={4: 0} if more else {},
        compiler_params=pltpu.CompilerParams(vmem_limit_bytes=VMEM_LIMIT),
        cost_estimate=cost((da.shape[0] + db.shape[0]) * d * v, 4 * da.shape[0] * v))(da, db, xa, xb, *more)


def weight_body(h_ref, g_ref, o_ref):
    o_ref[...] = lax.dot_general(h_ref[...], g_ref[...], TN, preferred_element_type=F32)


def weight_call(h, g):
    t, d = h.shape
    tv = 256
    return pl.pallas_call(
        weight_body, grid=(d // tv,),
        in_specs=[pl.BlockSpec((t, tv), lambda j: (0, j)),
                  once((t, d))],
        out_specs=pl.BlockSpec((tv, d), lambda j: (j, 0)), out_shape=jax.ShapeDtypeStruct((d, d), F32),
        compiler_params=pltpu.CompilerParams(vmem_limit_bytes=VMEM_LIMIT),
        cost_estimate=cost(2 * t * d * d, 4 * d * d))(h, g)


def share_body(at, own, core, other, *rest):
    outs, scr = rest[:-1], rest[-1]
    scr[...] = own[...] + core[...] + other[...]
    for k, out in enumerate(outs):
        out[...] = scr[pl.ds(pl.multiple_of(at[k], 8), out.shape[0]), :]


def share_call(at, own, from_core, from_y, wide):
    n, d = own.shape
    return pl.pallas_call(
        share_body,
        grid_spec=pltpu.PrefetchScalarGridSpec(
            num_scalar_prefetch=1, grid=(1,),
            in_specs=[fixed((n, d)), pl.BlockSpec((n, d), lambda i, p: (1, 0)), fixed((n, d))],
            out_specs=[fixed((wide, d))] * 4, scratch_shapes=[pltpu.VMEM((n, d), F32)]),
        out_shape=[jax.ShapeDtypeStruct((wide, d), F32)] * 4,
        compiler_params=pltpu.CompilerParams(vmem_limit_bytes=VMEM_LIMIT),
        cost_estimate=cost(n * d * 2000, n * d * 20))(at, own, from_core, from_y)


def norm_back_body(*refs):
    l4, r4, pick, (a_ref, g_ref, da_ref, db_ref) = refs[:4], refs[4:8], refs[8:-4], refs[-4:]
    halves = [(p[0][...] + p[1][...]) + (p[2][...] + p[3][...]) for p in (l4, r4)]
    dy = jnp.concatenate(halves, axis=1)
    for sel in pick:
        dy = jnp.dot(sel[...], dy, precision=lax.Precision.HIGHEST, preferred_element_type=F32)
    a = a_ref[...].astype(F32)
    cen = a - row_mean(a)
    inv = lax.rsqrt(row_mean(cen * cen) + LN_EPS)
    hat = cen * inv
    dh = dy * g_ref[...]
    da = inv * (dh - row_mean(dh) - hat * row_mean(dh * hat))
    da_ref[...] = da
    db_ref[...] = da.astype(BF)


def norm_back(parts, pick, a, gain):
    t, d = a.shape
    vm = pl.BlockSpec(memory_space=pltpu.VMEM)
    return pl.pallas_call(
        norm_back_body, in_specs=[vm] * (10 + len(pick)), out_specs=[vm] * 2,
        out_shape=[jax.ShapeDtypeStruct((t, d), F32), jax.ShapeDtypeStruct((t, d), BF)],
        compiler_params=pltpu.CompilerParams(vmem_limit_bytes=24 * 1024 * 1024),
        cost_estimate=cost(1_000_000_000, 22 * t * d))(*parts, *pick, a, gain)


SIZES = ((1280, 384, 128), (1536, 448, 128), (2048, 512, 136))


def solution(mesh):
    tok_spec = P(('dp', 'tp'), None)
    row_spec = P(None, ('dp', 'tp'))

    def device_step(hidden, w_two, ln_scale, ln_shift, embed, targets, loss_mask):
        h_all, ints = row_gather(hidden, 1, jnp.concatenate([targets, loss_mask, jnp.zeros((4, targets.shape[1]), jnp.int32)], axis=0), 1)
        shares = jnp.sum(ints[:, :, :, 2:4], axis=-1)
        share_max = jnp.max(shares[..., 0])
        quarter_max = jnp.max(jnp.sum(shares[..., 0], axis=2))
        all_max = jnp.max(jnp.sum(shares[..., 1], axis=(1, 2)))
        fits = [(all_max <= rows) & (quarter_max <= cap) & (share_max + 7 <= wide) for rows, cap, wide in SIZES[:-1]]
        which = jnp.where(fits[0], 0, jnp.where(fits[1], 1, 2))
        args = (hidden, w_two, ln_scale, ln_shift, embed, h_all, ints[lax.axis_index('dp')])
        return lax.switch(which, [functools.partial(branch, n) for n in range(len(SIZES))], *args)

    def branch(n, *args):
        return step(n, *SIZES[n], *args)

    def step(num, cap_b, cap_a, wide_a, hidden, w_two, ln_scale, ln_shift, embed, h_all, ints):
        toks, width = hidden.shape
        span = 4 * toks
        cid = 10 * (num + 1)
        base = (lax.axis_index('tp') * embed.shape[0]).astype(F32)
        zi, yi, ci = place()
        mine = 2 * ci + yi
        ring = lax.rem(zi + jnp.arange(4, dtype=jnp.int32), 4)
        perm = jnp.stack([3 - mine, 2 * (1 - ci) + yi, 2 * ci + 1 - yi, mine])
        h_rows = h_all.reshape(4 * span, width)
        tri = (lax.broadcasted_iota(jnp.int32, (span, span), 0) < lax.broadcasted_iota(jnp.int32, (span, span), 1)).astype(BF)
        caps = (cap_a, cap_b // 4)

        def compact(h):
            cap = caps[h]
            mask = ints[:, :, 2 + h].reshape(4, span)
            rank = jnp.dot(mask.astype(BF), tri, preferred_element_type=F32).astype(jnp.int32)
            starts = rank[:, ::toks]
            count = jnp.sum(mask, axis=1)
            if h == 1:
                rank = rank + (jnp.cumsum(count) - count)[:, None]
            slot = jnp.where(mask > 0, rank, -1)
            row = lax.broadcasted_iota(jnp.int32, (4, cap, 1), 1)
            if h == 1:
                row = row + lax.broadcasted_iota(jnp.int32, (4, cap, 1), 0) * cap
                pick = (row.reshape(4 * cap, 1) == slot.reshape(1, -1)).astype(BF)
                contract = lambda rhs: jnp.dot(pick, rhs.reshape(4 * span, -1), preferred_element_type=F32).reshape(4, cap, -1)
            else:
                pick = (row == slot[:, None, :]).astype(BF)
                contract = lambda rhs: jnp.einsum('qrt,qtd->qrd', pick, rhs.reshape(4, span, -1), preferred_element_type=F32)
            tgt = ints[:, :, h].reshape(4, span)
            vals = jnp.stack([mask, lax.div(tgt, 256), lax.rem(tgt, 256)], axis=-1).astype(BF)
            got = jnp.swapaxes(contract(vals), 1, 2)
            got = jnp.pad(got, ((0, 0), (0, 0), (0, 512 - cap)))
            wgt = got[:, 0] / jnp.sum(count).astype(F32)
            tgt_row = got[:, 1] * 256.0 + got[:, 2] - base
            rows = contract(h_rows).astype(BF).reshape(4 * cap, width)
            return slot, starts, rows, wgt, tgt_row

        def pad8(*rows):
            return jnp.stack(list(rows) + [jnp.zeros_like(rows[0])] * (8 - len(rows)), axis=1)

        def statistics(h, rows, tgt_row, wgt):
            z, st, x = logits_call(rows, embed, pad8(tgt_row), jnp.stack([ln_scale[h], ln_shift[h]]))
            s = jnp.where(st[:, 1] > 0.0, st[:, 1], 1.0)
            part = jnp.concatenate([(st[:, 0] + jnp.log(s)).reshape(16, 128), st[:, 2].reshape(16, 128)], axis=0)
            parts = small_gather(part, cid + h).reshape(16, 2, 4, 512)
            top = jnp.max(parts[:, 0], axis=0)
            lse = top + jnp.log(jnp.sum(jnp.exp(parts[:, 0] - top), axis=0))
            return x, z, pad8(lse, wgt, tgt_row, st[:, 3], st[:, 4]), lse - jnp.sum(parts[:, 1], axis=0)

        def own_slots(slot):
            return lax.dynamic_slice_in_dim(slot[mine], zi * toks, toks)

        def own_rows(h, slot):
            own = own_slots(slot)
            return jnp.where(own >= 0, own + (mine * caps[0] if h == 0 else 0), -1)

        def losses(h, slot, raw, wgt):
            flat = raw[:, :caps[h]].reshape(1, -1)
            hit = own_rows(h, slot)[:, None] == lax.broadcasted_iota(jnp.int32, (toks, flat.shape[1]), 1)
            return jnp.sum(jnp.where(hit, flat, 0.0), axis=1), jnp.sum(raw * wgt)

        def exchange(begins, wide, to_core, to_y, own):
            n = own.shape[0]
            from_core = lax.ppermute(to_core, 'tp', CORE_PAIRS)
            send = to_y + from_core[:n]
            from_y = lax.ppermute(send, 'tp', Y_PAIRS)
            parts = list(share_call(begins, own, from_core, from_y, wide))
            for k in Z_PAIRS:
                parts[k] = lax.ppermute(parts[k], 'tp', Z_PAIRS[k])
            return parts

        def halves(z, rows8, hid, begins, wide):
            dz, *left, sum_l = grad_call(1, z, embed, rows8, hid, perm)
            *right, sum_r = grad_call(0, dz, embed, rows8, hid, perm)
            return dz, exchange(begins, wide, *left) + exchange(begins, wide, *right), right[2], jnp.concatenate([sum_l, sum_r], axis=1)

        slot_b, _, hid_b, wgt_b, tgt_b = compact(1)
        proj_b = jnp.dot(hid_b, w_two, preferred_element_type=F32).astype(BF)
        x_b, z_b, rows_b, raw_b = statistics(1, proj_b, tgt_b, wgt_b)
        loss_b, tot_b = losses(1, slot_b, raw_b, wgt_b)
        wide_b = cap_b // 16
        dz_b, parts_b, last_b, sums_b = halves(z_b, rows_b, proj_b, ring * wide_b, wide_b)

        slot_a, starts_a, hid_a, wgt_a, tgt_a = compact(0)
        hid_a, slot_a, starts_a, _ = lax.optimization_barrier((hid_a, slot_a, starts_a, last_b))
        starts_a = jnp.minimum(starts_a - lax.rem(starts_a, 8), cap_a - wide_a)[mine]
        begins_a = jnp.take(starts_a, ring)
        at = own_slots(slot_a)
        at = jnp.where(at >= 0, at - begins_a[0], -1)
        pick_a = (at[:, None] == lax.broadcasted_iota(jnp.int32, (toks, wide_a), 1)).astype(F32)
        hid_a, begins_a, pick_a = lax.optimization_barrier((hid_a, begins_a, pick_a))
        x_a, z_a, rows_a, raw_a = statistics(0, hid_a, tgt_a, wgt_a)
        loss_a, tot_a = losses(0, slot_a, raw_a, wgt_a)
        dz_a, parts_a, _, sums_a = halves(z_a, rows_a, hid_a, begins_a, wide_a)
        d_embed = embed_call(dz_a, dz_b, x_a, x_b, 0)
        d_embed = embed_call(dz_a, dz_b, x_a, x_b, 1, d_embed)

        own_b = lax.dynamic_slice_in_dim(proj_b, mine * caps[1] + zi * wide_b, wide_b)
        _, d_proj = norm_back(parts_b, [], own_b, ln_scale[1:2])
        ln_part = jnp.concatenate([v.reshape(-1, 128) for v in (sums_a[0], sums_b[0], sums_a[1], sums_b[1])], axis=0)
        g_all, ln_all = row_gather(d_proj, cid + 2, ln_part, 0)
        g_all = g_all.reshape(cap_b, width)
        ln_all = jnp.sum(ln_all.reshape(16, 4, width), axis=0)
        d_w_two = weight_call(hid_b, g_all)
        pick_b = (own_rows(1, slot_b)[:, None] == lax.broadcasted_iota(jnp.int32, (toks, cap_b), 1)).astype(BF)
        d_own = jnp.dot(pick_b, g_all, preferred_element_type=F32).astype(BF)
        via_two = lax.dot_general(d_own, w_two, NT, preferred_element_type=F32)
        da_a, _ = norm_back(parts_a, [pick_a], hidden, ln_scale[0:1])
        d_hidden = (da_a + via_two).astype(BF)
        token_loss = jnp.stack([loss_a, loss_b])
        return token_loss, (tot_a + tot_b).reshape(1), d_hidden, d_embed, d_w_two, ln_all[:2], ln_all[2:]

    return jax.shard_map(device_step, mesh=mesh,
                         in_specs=(tok_spec, P(), P(), P(), P('tp', None), row_spec, row_spec),
                         out_specs=(row_spec, P('dp'), tok_spec, tok_spec, P('dp', None), P('dp', None), P('dp', None)),
                         check_vma=False)
```
